32 devices in a mesh: seq: 8 (over z, y), tp: 4 (over x, core).
Axes of the slice: x: 2, y: 2, z: 4, core: 2. Of those that a mesh axis runs over, the one named last changes fastest.
Arguments:
- tokens: bfloat16 [6144, 4096], P('seq'), may hold values from -6 to 6
- query_weight: bfloat16 [4096, 2048], P('seq', 'tp'), may hold values from -0.09375 to 0.09375
- key_weight: bfloat16 [4096, 2048], P('seq', 'tp'), may hold values from -0.09375 to 0.09375
- value_weight: bfloat16 [4096, 2048], P('seq', 'tp'), may hold values from -0.09375 to 0.09375
- gate_weight: bfloat16 [4096, 16], P('seq', 'tp'), may hold values from -0.09375 to 0.09375
- decay_rate: float32 [16], P('tp'), may hold values from 3.2552085e-05 to 0.04
- norm_gain: float32 [2048], P('tp'), may hold values from 0.5 to 1.5
- out_weight: bfloat16 [2048, 4096], P(None, 'tp'), may hold values from -0.125 to 0.125
Outputs:
- mixed: bfloat16 [6144, 4096], P('seq', 'tp')
The draws below stay inside these ranges and needn't reach their ends.
All inputs are finite; a program needn't handle non-finite values.
Results may differ from the reference program's by a relative error of at most 0.006.
The reference program's roundings to bfloat16 on the way count: a program that leaves them out, or rounds other values in their place, can miss the bound.
Values may be sent and summed in bfloat16 or wider, within the bound.
A program may use at most 128 MiB of HBM per device.

```python
import math
import jax
import jax.numpy as jnp
from jax import lax

D = 4096
H = 16
K = 128
TOK_DEV = 768
TOKENS = 6144


def level_of(own_key, shape, shards, smallest, high):
    def one(dim, blocks):
        steps = jax.random.uniform(jax.random.fold_in(jax.random.fold_in(own_key, 6), dim), (blocks,), jnp.float32, smallest / len(shards), high / len(shards))
        return jnp.repeat(jnp.exp(steps), shape[dim] // blocks).reshape((-1,) + (1,) * (len(shape) - dim - 1))

    level = one(*shards[0])
    for cut in shards[1:]:
        level = level * one(*cut)
    return level


def centred(own_key, dims, spread, reach, pieces=(), kind=jnp.bfloat16):
    loudness = level_of(own_key, dims, pieces, -0.22, 0.18) if pieces else 1.0
    values = jax.random.normal(own_key, dims, jnp.float32) * spread * loudness
    return jnp.minimum(jnp.maximum(values, -reach), reach).astype(kind)


def setup_inputs(seed: int = 0) -> dict:
    key_of = jax.random.split(jax.random.key(seed), 9)
    return {
        "tokens": centred(key_of[0], (TOKENS, D), 1.0, 6.0, ((0, 8),)),
        "query_weight": centred(key_of[1], (D, H * K), D ** -0.5, 0.09375, ((0, 8), (1, 4))),
        "key_weight": centred(key_of[2], (D, H * K), D ** -0.5, 0.09375, ((0, 8), (1, 4))),
        "value_weight": centred(key_of[3], (D, H * K), D ** -0.5, 0.09375, ((0, 8), (1, 4))),
        "gate_weight": centred(key_of[4], (D, H), D ** -0.5, 0.09375, ((0, 8), (1, 4))),
        "decay_rate": jnp.clip(jnp.exp(math.log(0.04) - 7.1137933 * jax.random.uniform(key_of[5], (H,), jnp.float32) ** level_of(key_of[5], (H,), ((0, 4),), -0.2, 0.2)), 3.255208503105678e-05, 0.04),
        "norm_gain": jnp.clip(1.0 + 0.1 * jax.random.normal(key_of[6], (H * K,), jnp.float32), 0.5, 1.5),
        "out_weight": centred(key_of[7], (H * K, D), (H * K) ** -0.5, 0.125, ((1, 4),)),
    }


def reference(tokens, query_weight, key_weight, value_weight, gate_weight, decay_rate, norm_gain, out_weight):
    query_proj = jnp.dot(tokens, query_weight, preferred_element_type=jnp.float32).astype(jnp.bfloat16)
    key_proj = jnp.dot(tokens, key_weight, preferred_element_type=jnp.float32).astype(jnp.bfloat16)
    value_proj = jnp.dot(tokens, value_weight, preferred_element_type=jnp.float32).astype(jnp.bfloat16)
    gate_logit = jnp.dot(tokens, gate_weight, preferred_element_type=jnp.float32)
    log_decay = -decay_rate[None, :] * jax.nn.softplus(gate_logit)
    block_count = TOKENS // TOK_DEV
    query_blocks = query_proj.reshape(block_count, TOK_DEV, H, K)
    key_blocks = key_proj.reshape(block_count, TOK_DEV, H, K)
    value_blocks = value_proj.reshape(block_count, TOK_DEV, H, K)
    decay_blocks = log_decay.reshape(block_count, TOK_DEV, H)
    causal = jnp.tril(jnp.ones((TOK_DEV, TOK_DEV), dtype=bool))[None, :, :]

    def block_step(prev_state, items):
        query_blk, key_blk, value_blk, decay_blk = items
        within = jnp.cumsum(decay_blk, axis=0)
        block_total = within[-1]
        query_wide = query_blk.astype(jnp.float32)
        key_wide = key_blk.astype(jnp.float32)
        value_full_width = value_blk.astype(jnp.float32)
        query_scaled = (jnp.exp(within)[:, :, None] * query_wide).astype(jnp.bfloat16)
        state_bfloat = prev_state.astype(jnp.bfloat16)
        carried_state = jnp.einsum('fys,ysu->fyu', query_scaled.astype(jnp.float32), state_bfloat.astype(jnp.float32))
        scores = jnp.einsum('thk,shk->hts', query_wide, key_wide)
        decay_gap = within.T[:, :, None] - within.T[:, None, :]
        attn = jnp.where(causal, scores * jnp.exp(jnp.where(causal, decay_gap, 0.0)), 0.0).astype(jnp.bfloat16)
        local_part = jnp.einsum('hts,shv->thv', attn.astype(jnp.float32), value_full_width)
        key_scaled = (jnp.exp(block_total[None, :] - within)[:, :, None] * key_wide).astype(jnp.bfloat16)
        shard_local_state = jnp.einsum('gfw,gfz->fwz', key_scaled.astype(jnp.float32), value_full_width)
        next_state = jnp.exp(block_total)[:, None, None] * prev_state + shard_local_state
        return (next_state, carried_state + local_part)
    start_state = jnp.zeros((H, K, K), jnp.float32)
    _, head_out = lax.scan(block_step, start_state, (query_blocks, key_blocks, value_blocks, decay_blocks))
    mean_square = lax.optimization_barrier(jnp.mean(head_out * head_out, axis=-1, keepdims=True))
    normed = (head_out * lax.rsqrt(mean_square + 1e-05)).reshape(TOKENS, H * K) * norm_gain[None, :]
    normed = normed.astype(jnp.bfloat16)
    return jnp.dot(normed, out_weight, preferred_element_type=jnp.float32).astype(jnp.bfloat16)
```

```python
import functools

import jax
import jax.numpy as jnp
from jax import lax
from jax.experimental import pallas as pl
from jax.experimental.pallas import tpu as pltpu
from jax.sharding import PartitionSpec as P

HALVES = 2
MESH = pl.DeviceIdType.MESH
CROSS = 2
PHASES = [[1, 0, 2], [4], [5], [3], [6], [7]]
EARLY = (3, 4, 5, 6, 7)
PARTS = 8


def layer_kernel(seq, tp, heads, wide, *refs):
    tok_in, rate_ref, gain_ref, gate_in, key_in, value_in, query_in, out_in = refs[:8]
    mixed_ref = refs[8]
    gate_buf, kvq_buf, gate_acc, acc, out_buf, out_acc, wcol, wrow = refs[9:17]
    state_mine, state_wire, state_peer, total_mine, total_peer = refs[17:22]
    state_in, state_next, state_pre, normed_buf, tok_ref = refs[22:27]
    own_sem, send_own, send_line, send_peer, recv_sem = refs[27:32]
    tok_send, tok_recv, local_send, local_recv, state_send, state_recv = refs[32:38]
    normed_send, normed_recv, guest_send = refs[38:41]
    rows = key_in.shape[0]
    half = key_in.shape[1] // HALVES
    quarter = half // 2
    line = seq // CROSS
    me = lax.axis_index("seq")
    a, b = me // CROSS, me % CROSS
    peer = a * CROSS + (1 - b)
    count = acc.shape[1] // 2
    head_size = 2 * half // heads
    per_half = heads // HALVES
    block = 256 if count % 256 == 0 else count
    blocks = count // block
    col = lax.axis_index("tp")
    pair_col = col + 1 - 2 * (col % 2)
    groups = tp // 2
    last = line - 1
    is_end = (a == 0) | (a == last)
    is_worker = (a > 0) & (a < last)
    all_hosts = line == 4
    is_host = (a == 1) | (a == last - 1)
    is_low = a == 1
    up_works, down_works = a + 1 < last, a - 1 > 0
    partner = jnp.where((a == 0) | ((a == last - 1) & (a != 1)), me + CROSS, me - CROSS)
    units = [
        (0, 0, half, range(per_half)),
        (1, 0, quarter, range(per_half // 2)),
        (1, quarter, quarter, range(per_half // 2, per_half)),
    ]

    def hosts(run):
        if all_hosts:
            run()
        else:
            pl.when(is_host)(run)

    def buffer(piece, source):
        if piece == 0:
            return gate_buf.at[source]
        if piece >= 3 * HALVES:
            at = pl.ds((piece - 3 * HALVES) * quarter, quarter)
            return kvq_buf.at[3 * HALVES - 1, source, :, at]
        return kvq_buf.at[piece - 1, source]

    def copy(piece, source, sem, target):
        return pltpu.make_async_remote_copy(
            src_ref=buffer(piece, source),
            dst_ref=buffer(piece, source),
            send_sem=sem,
            recv_sem=recv_sem.at[piece, source],
            device_id={"seq": target},
            device_id_type=MESH,
        )

    def arrive(piece, source):
        copy(piece, source, send_own.at[piece, 0], peer).wait_recv()

    loads = [pltpu.make_async_copy(gate_in, gate_buf.at[me], own_sem.at[0])]
    for index in range(3 * HALVES):
        source_ref = (key_in, value_in, query_in)[index % 3]
        at = (index // 3) * half
        loads.append(
            pltpu.make_async_copy(
                source_ref.at[:, pl.ds(at, half)], kvq_buf.at[index, me], own_sem.at[index + 1]
            )
        )
    for load in loads:
        load.start()
    if wide:
        own_tok = tok_ref.at[pl.ds(0, count), :]
    else:
        own_tok = tok_ref.at[:, pl.ds(0, count), :]
    tok_load = pltpu.make_async_copy(tok_in, own_tok, own_sem.at[3 * HALVES + 2])
    tok_load.start()
    out_load = pltpu.make_async_copy(out_in, out_buf, own_sem.at[3 * HALVES + 1])
    out_load.start()

    barrier = pltpu.get_barrier_semaphore()
    has_up, has_down = a < last, a > 0
    pl.semaphore_signal(barrier, inc=1, device_id={"seq": peer}, device_id_type=MESH)

    @pl.when(has_up)
    def _():
        pl.semaphore_signal(barrier, inc=1, device_id={"seq": me + CROSS}, device_id_type=MESH)

    @pl.when(has_down)
    def _():
        pl.semaphore_signal(barrier, inc=1, device_id={"seq": me - CROSS}, device_id_type=MESH)

    pl.semaphore_signal(barrier, inc=1, device_id={"tp": pair_col}, device_id_type=MESH)
    for g in range(1, groups):
        pl.semaphore_signal(
            barrier, inc=1, device_id={"tp": lax.rem(col + 2 * g, tp)}, device_id_type=MESH
        )
    pl.semaphore_wait(barrier, 1 + groups + has_up.astype(jnp.int32) + has_down.astype(jnp.int32))

    def load_wait(piece):
        if piece <= 3 * HALVES:
            loads[piece].wait()

    def far(g):
        return lax.rem(col + 2 * g, tp)

    def far_pair(g):
        return lax.rem(pair_col + 2 * g, tp)

    def own_line(number):
        for piece in PHASES[number]:

            @pl.when(up_works)
            def _():
                copy(piece, me, send_own.at[piece, 1], me + CROSS).start()

            @pl.when(down_works)
            def _():
                copy(piece, me, send_own.at[piece, 2], me - CROSS).start()

    def own_cross(number):
        for piece in PHASES[number]:
            copy(piece, me, send_own.at[piece, 0], peer).start()

    def each_middle(run):
        @pl.loop(1, line - 2)
        def _(d):
            for sign in (1, -1):
                origin = a - sign * d
                onward = up_works if sign == 1 else down_works

                @pl.when((origin > 0) & (origin < last))
                def _():
                    run(origin, onward, me + sign * CROSS)

    near_low = 2 * a < line
    near_origin = jnp.where(near_low, 0, last)
    far_origin = last - near_origin
    near_onward = jnp.where(near_low, up_works, down_works)
    far_onward = jnp.where(near_low, down_works, up_works)
    away = jnp.where(near_low, CROSS, -CROSS)

    def ends():
        return (near_origin, near_onward, me + away), (far_origin, far_onward, me - away)

    def middle(number):
        def run(origin, onward, target):
            source = origin * CROSS + b
            for piece in PHASES[number]:
                arrive(piece, source)
                copy(piece, source, send_peer.at[piece, source], peer).start()

                @pl.when(onward)
                def _():
                    copy(piece, source, send_line.at[piece, source], target).start()

        each_middle(run)

    def outer(number, which):
        origin, onward, target = ends()[which]
        source, other = origin * CROSS + b, origin * CROSS + (1 - b)
        for piece in PHASES[number]:
            arrive(piece, source)

            @pl.when(onward)
            def _():
                copy(piece, source, send_line.at[piece, source], target).start()

            if piece in EARLY:
                arrive(piece, other)

                @pl.when(onward)
                def _():
                    copy(piece, other, send_line.at[piece, other], target).start()

            else:
                copy(piece, source, send_peer.at[piece, source], peer).start()

    def tok_part(ref, index, base):
        if wide:
            size = ref.shape[1] // (tp * PARTS)
            at = pl.ds(pl.multiple_of(index * size, size), size)
            return ref.at[pl.ds(base, count), at]
        size = seq // (tp * PARTS)
        return ref.at[pl.ds(index * size, size), pl.ds(base, count), :]

    def tok_copy(index, j, send, target, first=False):
        return pltpu.make_async_remote_copy(
            src_ref=tok_part(tok_in, index, 0) if first else tok_part(tok_ref, index, count),
            dst_ref=tok_part(tok_ref, index, count),
            send_sem=tok_send.at[j, send],
            recv_sem=tok_recv.at[index],
            device_id=target,
            device_id_type=MESH,
        )

    def tok_arrive(index):
        tok_copy(index, 0, 0, {"tp": pair_col}).wait_recv()

    def tok_spread(j):
        def run():
            index = col * PARTS + j
            tok_arrive(index)
            for g in range(1, groups):
                tok_copy(index, j, g, {"tp": far(g)}).start()
            tok_copy(index, j, 0, {"tp": pair_col}).start()

        hosts(run)

    def tok_relay(j):
        def run():
            for g in range(1, groups):
                index = far(g) * PARTS + j
                tok_arrive(index)
                tok_copy(index, j, groups - 1 + g, {"tp": pair_col}).start()

        hosts(run)

    def tok_rest():
        def run():
            for j in range(PARTS):
                tok_arrive(pair_col * PARTS + j)
                for g in range(1, groups):
                    tok_arrive(far_pair(g) * PARTS + j)

        hosts(run)

    def multiply(piece, source, base, size):
        at = slice(base, base + size)
        if wide:
            x = tok_ref[at, pl.ds(pl.multiple_of(source * rows, rows), rows)]
        else:
            x = tok_ref[source, at]
        if piece == 0:
            gate_acc[at] += lax.dot_general(
                x, gate_buf[source], (((1,), (1,)), ((), ())), preferred_element_type=jnp.float32
            )
        elif piece >= 3 * HALVES:
            cols = slice((piece - 3 * HALVES) * quarter, (piece - 3 * HALVES + 1) * quarter)
            acc[3 * HALVES - 1, at, cols] += jnp.dot(
                x, kvq_buf[3 * HALVES - 1, source, :, cols], preferred_element_type=jnp.float32
            )
        else:
            acc[piece - 1, at] += jnp.dot(
                x, kvq_buf[piece - 1, source], preferred_element_type=jnp.float32
            )

    def product(piece, source, part):
        if part == "own":
            multiply(piece, source, 0, count)
        elif part == "guest":
            hosts(lambda: multiply(piece, source, count, count))
        elif all_hosts:
            multiply(piece, source, 0, 2 * count)
        else:

            @pl.when(is_host)
            def _():
                multiply(piece, source, 0, 2 * count)

            @pl.when(jnp.logical_not(is_host))
            def _():
                multiply(piece, source, 0, count)

    def mine(number, part):
        for piece in PHASES[number]:
            product(piece, me, part)

    def middles(number, part):
        def run(origin, onward, target):
            for piece in PHASES[number]:
                product(piece, origin * CROSS + b, part)

        each_middle(run)

    def outside(number, which, part):
        origin = ends()[which][0]
        for piece in PHASES[number]:
            product(piece, origin * CROSS + b, part)
            if piece in EARLY:
                product(piece, origin * CROSS + (1 - b), part)

    def crossed_mine(number, part):
        for piece in PHASES[number]:
            arrive(piece, peer)
            product(piece, peer, part)

    def crossed(number, part):
        pieces = PHASES[number]

        def run(origin, onward, target):
            for piece in pieces:
                source = origin * CROSS + (1 - b)
                arrive(piece, source)
                product(piece, source, part)

        each_middle(run)

    def crossed_outside(number, which, part):
        for piece in PHASES[number]:
            if piece not in EARLY:
                source = ends()[which][0] * CROSS + (1 - b)
                arrive(piece, source)
                product(piece, source, part)

    def guests(number, rest=True):
        pieces = PHASES[number]

        def run():
            if rest:

                @pl.loop(0, seq)
                def _(source):
                    for piece in pieces:
                        multiply(piece, source, count, count)

            else:

                @pl.loop(CROSS, seq - CROSS)
                def _(source):
                    for piece in pieces:
                        multiply(piece, source, count, count)

        hosts(run)

    trips = 2 if all_hosts else 1 + is_host.astype(jnp.int32)
    first_group = jnp.where(is_low, 1, 0)
    second_group = 1 - first_group

    def token_rows(w, start, size):
        return pl.ds(pl.multiple_of(w * count + start, block), size)

    def decays():
        @pl.loop(0, trips)
        def _(w):
            logits = jnp.concatenate(
                [
                    gate_acc[token_rows(w, 0, count)],
                    jnp.zeros((count, 128 - gate_acc.shape[1]), jnp.float32),
                ],
                axis=1,
            ).T[:8]
            soft = jnp.maximum(logits, 0.0) + jnp.log1p(jnp.exp(-jnp.abs(logits)))
            total = -rate_ref[...] * soft
            lane = lax.broadcasted_iota(jnp.int32, total.shape, 1)
            reach = 1
            while reach < count:
                total = total + jnp.where(lane >= reach, pltpu.roll(total, reach, 1), 0.0)
                reach *= 2
            wrow[w] = total
            wcol[w] = jnp.concatenate([total, jnp.zeros((120, count), jnp.float32)], axis=0).T

    class local_copy:
        def __init__(self, h, slot, group):
            pairs = ((state_wire, state_peer), (total_mine, total_peer))
            self.copies = [
                pltpu.make_async_remote_copy(
                    src_ref=source.at[group, h],
                    dst_ref=target.at[slot, h],
                    send_sem=local_send.at[n, slot, h],
                    recv_sem=local_recv.at[n, slot, h],
                    device_id={"seq": peer},
                    device_id_type=MESH,
                )
                for n, (source, target) in enumerate(pairs)
            ]

        def start(self):
            for one in self.copies:
                one.start()

        def wait_recv(self):
            for one in self.copies:
                one.wait_recv()

        def wait_send(self):
            for one in self.copies:
                one.wait_send()

    def local_state(h):
        @pl.loop(0, trips)
        def _(w):
            for j in range(per_half):
                head = h * per_half + j
                cols = slice(j * head_size, (j + 1) * head_size)
                within = wcol[w, :, head : head + 1]
                final = wcol[w, count - 1 : count, head : head + 1]
                at = token_rows(w, 0, count)
                key = acc[3 * h, at, cols].astype(jnp.bfloat16).astype(jnp.float32)
                scaled = (jnp.exp(final - within) * key).astype(jnp.bfloat16)
                value = acc[3 * h + 1, at, cols].astype(jnp.bfloat16)
                local = lax.dot_general(
                    scaled, value, (((0,), (0,)), ((), ())), preferred_element_type=jnp.float32
                )
                state_mine[w, h, j * head_size : (j + 1) * head_size] = local
                state_wire[w, h, j * head_size : (j + 1) * head_size] = local.astype(jnp.bfloat16)
                total_mine[w, h, j : j + 1] = jnp.broadcast_to(final, (1, head_size))

        local_copy(h, 0, first_group).start()
        hosts(lambda: local_copy(h, 1, second_group).start())

    def line_state(h):
        return pltpu.make_async_remote_copy(
            src_ref=state_next.at[h],
            dst_ref=state_in.at[h],
            send_sem=state_send.at[h],
            recv_sem=state_recv.at[h],
            device_id={"seq": me + CROSS},
            device_id_type=MESH,
        )

    def chain(h):
        @pl.when(is_low)
        def _():
            state_in[h] = jnp.zeros(state_in.shape[1:], jnp.float32)

        @pl.when(jnp.logical_not(is_low))
        def _():
            line_state(h).wait_recv()

        spans = [slice(j * head_size, (j + 1) * head_size) for j in range(per_half)]

        def step(state, j, slot, group, peers):
            own = (total_mine[group, h, j : j + 1], state_mine[group, h, spans[j]])
            other = (
                total_peer[slot, h, j : j + 1],
                state_peer[slot, h, spans[j]].astype(jnp.float32),
            )
            total = jnp.where(peers, other[0], own[0])
            return jnp.exp(total) * state + jnp.where(peers, other[1], own[1])

        def pass_group(slot, group):
            local_copy(h, slot, group).wait_recv()
            for j, at in enumerate(spans):
                state = state_in[h, at] if slot == 0 else state_next[h, at]
                middle_state = step(state, j, slot, group, b == 1)
                state_pre[group, h, at] = jnp.where(b == 1, middle_state, state).astype(
                    jnp.bfloat16
                )
                state_next[h, at] = step(middle_state, j, slot, group, b == 0)

        pass_group(0, first_group)
        hosts(lambda: pass_group(1, second_group))

        @pl.when(up_works)
        def _():
            line_state(h).start()

    def block_rows(i):
        return pl.ds(i * block if isinstance(i, int) else pl.multiple_of(i * block, block), block)

    def normed_copy(u, i, source, send, target):
        h, start, size, _ = units[u]
        ref = normed_buf.at[h, source, block_rows(i), pl.ds(start, size)]
        return pltpu.make_async_remote_copy(
            src_ref=ref,
            dst_ref=ref,
            send_sem=normed_send.at[u, i, send],
            recv_sem=normed_recv.at[u, i, source],
            device_id={"tp": target},
            device_id_type=MESH,
        )

    def guest_copy(u, i):
        h, start, size, _ = units[u]
        return pltpu.make_async_remote_copy(
            src_ref=normed_buf.at[h, tp, block_rows(i), pl.ds(start, size)],
            dst_ref=normed_buf.at[h, col, block_rows(i), pl.ds(start, size)],
            send_sem=guest_send.at[u, i],
            recv_sem=normed_recv.at[u, i, col],
            device_id={"seq": partner},
            device_id_type=MESH,
        )

    def share(u, i):
        for g in range(1, groups):
            normed_copy(u, i, col, g, far(g)).start()
        normed_copy(u, i, col, 0, pair_col).start()

    def relay(u, i):
        for g in range(1, groups):
            normed_copy(u, i, far(g), 0, pair_col).wait_recv()
            normed_copy(u, i, far(g), groups - 1 + g, pair_col).start()

    def attention(u):
        h, _, _, members = units[u]

        @pl.loop(0, trips)
        def _(n):
            w = trips - 1 - n
            slot = jnp.where(w == 0, col, tp)
            for i in range(blocks):
                upto = (i + 1) * block
                row = i * block + lax.broadcasted_iota(jnp.int32, (block, upto), 0)
                causal = lax.broadcasted_iota(jnp.int32, (block, upto), 1) <= row
                t_at = token_rows(w, i * block, block)
                s_at = token_rows(w, 0, upto)
                for j in members:
                    head = h * per_half + j
                    cols = slice(j * head_size, (j + 1) * head_size)
                    query = acc[3 * h + 2, t_at, cols].astype(jnp.bfloat16)
                    key = acc[3 * h, s_at, cols].astype(jnp.bfloat16)
                    value = acc[3 * h + 1, s_at, cols].astype(jnp.bfloat16)
                    within = wcol[w, i * block : (i + 1) * block, head : head + 1]
                    scores = lax.dot_general(
                        query, key, (((1,), (1,)), ((), ())), preferred_element_type=jnp.float32
                    )
                    gap = within - wrow[w, head : head + 1, :upto]
                    attn = jnp.where(causal, scores * jnp.exp(jnp.where(causal, gap, 0.0)), 0.0)
                    local = jnp.dot(
                        attn.astype(jnp.bfloat16), value, preferred_element_type=jnp.float32
                    )
                    scaled = (jnp.exp(within) * query.astype(jnp.float32)).astype(jnp.bfloat16)
                    state = state_pre[w, h, j * head_size : (j + 1) * head_size]
                    head_out = local + jnp.dot(scaled, state, preferred_element_type=jnp.float32)
                    square = jnp.mean(head_out * head_out, axis=-1, keepdims=True)
                    gain = gain_ref[:, head * head_size : (head + 1) * head_size]
                    normed_buf[h, slot, i * block : (i + 1) * block, cols] = (
                        head_out * lax.rsqrt(square + 1e-05) * gain
                    ).astype(jnp.bfloat16)

                @pl.when(w == 0)
                def _():
                    share(u, i)

                @pl.when(w == 1)
                def _():
                    guest_copy(u, i).start()

    def settle(h):
        mine = [u for u in range(len(units)) if units[u][0] == h]

        def mix(i, source):
            depth = pl.ds(pl.multiple_of((source * HALVES + h) * half, half), half)
            return jnp.dot(
                normed_buf[h, source, block_rows(i)],
                out_buf[depth, :],
                preferred_element_type=jnp.float32,
            )

        @pl.loop(0, blocks)
        def _(i):
            at = block_rows(i)
            total = mix(i, col)
            for u in mine:
                normed_copy(u, i, pair_col, 0, pair_col).wait_recv()
            total = total + mix(i, pair_col)
            for g in range(1, groups):
                total = total + mix(i, far(g))
                for u in mine:
                    normed_copy(u, i, far_pair(g), 0, pair_col).wait_recv()
                total = total + mix(i, far_pair(g))
            if h == 0:
                out_acc[at, :] = total
            else:
                mixed_ref[at, :] = (out_acc[at, :] + total).astype(jnp.bfloat16)

    def relays(u):
        @pl.loop(0, blocks)
        def _(i):
            relay(u, i)

    @pl.when(is_end)
    def _():
        for pieces in PHASES:
            for piece in pieces:
                load_wait(piece)
                if piece in EARLY:
                    copy(piece, me, send_own.at[piece, 0], peer).start()
        for j in range(PARTS):
            tok_copy(col * PARTS + j, j, 0, {"seq": partner}, True).start()
        for pieces in PHASES:
            for piece in pieces:
                copy(piece, me, send_own.at[piece, 1], partner).start()
                if piece in EARLY:
                    arrive(piece, peer)
                    copy(piece, peer, send_line.at[piece, peer], partner).start()
        tok_load.wait()
        out_load.wait()
        for u in range(len(units)):

            @pl.loop(0, blocks)
            def _(i):
                guest_copy(u, i).wait_recv()
                share(u, i)

            relays(u)
            if u == 0:
                settle(0)

    @pl.when(is_worker)
    def _():
        gate_acc[...] = jnp.zeros_like(gate_acc)
        acc[...] = jnp.zeros_like(acc)
        for pieces in PHASES:
            for piece in pieces:
                load_wait(piece)
        tok_load.wait()
        own_cross(0)
        own_line(0)
        middle(0)
        mine(3, "own")
        middles(0, "own")
        own_line(1)
        own_line(2)
        own_cross(1)
        own_line(3)
        tok_spread(0)
        middle(1)
        tok_spread(1)
        crossed_mine(0, "own")
        mine(1, "own")
        tok_spread(2)
        tok_relay(0)
        crossed_mine(1, "own")
        own_line(4)
        tok_spread(3)
        own_cross(2)
        tok_spread(4)
        tok_spread(5)
        tok_relay(1)
        mine(0, "own")
        own_line(5)
        tok_relay(2)
        mine(5, "own")
        mine(2, "own")
        mine(4, "own")
        tok_spread(6)
        tok_relay(3)
        middle(2)
        outer(0, 0)
        outside(0, 0, "own")
        middles(1, "own")
        tok_spread(7)
        tok_relay(4)
        crossed(0, "own")
        tok_relay(5)
        tok_relay(6)
        middles(2, "own")
        crossed(1, "own")
        crossed_mine(2, "own")
        outer(0, 1)
        tok_relay(7)
        middle(3)
        outside(0, 1, "own")
        outer(1, 0)
        crossed(2, "own")
        crossed_outside(0, 0, "own")
        tok_rest()
        guests(1, False)
        own_cross(3)
        middles(3, "own")
        outside(1, 0, "both")
        guests(2, False)
        middle(4)
        middles(4, "own")
        outer(2, 0)
        outside(2, 0, "both")
        crossed_outside(0, 1, "own")
        outer(1, 1)
        guests(0)
        outer(3, 0)
        decays()
        local_state(0)
        crossed(3, "own")
        crossed_mine(3, "own")
        guests(3, False)
        outside(1, 1, "both")
        outside(3, 0, "both")
        chain(0)
        outer(2, 1)
        outer(4, 0)
        outer(3, 1)
        outside(3, 1, "both")
        attention(0)
        own_cross(4)
        outside(2, 1, "both")
        outer(5, 0)
        local_state(1)
        own_cross(5)
        middle(5)
        middles(5, "own")
        outside(4, 0, "both")
        crossed_mine(4, "own")
        crossed(4, "own")
        outer(4, 1)
        outside(4, 1, "both")
        guests(4, False)
        chain(1)
        attention(1)
        outside(5, 0, "both")
        relays(0)
        crossed_mine(5, "own")
        outer(5, 1)
        outside(5, 1, "both")
        crossed(5, "own")
        guests(5, False)
        attention(2)
        out_load.wait()
        settle(0)
        relays(1)
        relays(2)
    settle(1)

    @pl.loop(0, blocks)
    def _(i):
        for u in range(len(units)):
            for k in range(tp - 1):
                normed_copy(u, i, col, k, pair_col).wait_send()

    @pl.when(is_end)
    def _():
        for pieces in PHASES:
            for piece in pieces:
                copy(piece, me, send_own.at[piece, 1], peer).wait_send()
                if piece in EARLY:
                    copy(piece, me, send_own.at[piece, 0], peer).wait_send()
                    copy(piece, peer, send_line.at[piece, peer], peer).wait_send()
        for j in range(PARTS):
            tok_copy(col * PARTS + j, j, 0, {"seq": partner}, True).wait_send()

    @pl.when(is_worker)
    def _():
        def host_drain():
            for j in range(PARTS):
                for k in range(tp - 1):
                    tok_copy(col * PARTS + j, j, k, {"tp": pair_col}).wait_send()

            @pl.loop(0, blocks)
            def _(i):
                for u in range(len(units)):
                    guest_copy(u, i).wait_send()

        hosts(host_drain)
        for h in range(HALVES):

            local_copy(h, 0, first_group).wait_send()
            hosts(lambda: local_copy(h, 1, second_group).wait_send())

            @pl.when(up_works)
            def _():
                line_state(h).wait_send()

        for pieces in PHASES:
            for piece in pieces:
                copy(piece, me, send_own.at[piece, 0], peer).wait_send()

                @pl.when(up_works)
                def _():
                    copy(piece, me, send_own.at[piece, 1], peer).wait_send()

                @pl.when(down_works)
                def _():
                    copy(piece, me, send_own.at[piece, 2], peer).wait_send()

                for origin, onward, _ in ends():
                    source, other = origin * CROSS + b, origin * CROSS + (1 - b)

                    @pl.when(onward)
                    def _():
                        copy(piece, source, send_line.at[piece, source], peer).wait_send()
                        if piece in EARLY:
                            copy(piece, other, send_line.at[piece, other], peer).wait_send()

                    if piece not in EARLY:
                        copy(piece, source, send_peer.at[piece, source], peer).wait_send()

        def run(origin, onward, target):
            source = origin * CROSS + b
            for pieces in PHASES:
                for piece in pieces:
                    copy(piece, source, send_peer.at[piece, source], peer).wait_send()

                    @pl.when(onward)
                    def _():
                        copy(piece, source, send_line.at[piece, source], peer).wait_send()

        each_middle(run)


def on_device(
    seq,
    tp,
    tokens,
    query_weight,
    key_weight,
    value_weight,
    gate_weight,
    decay_rate,
    norm_gain,
    out_weight,
):
    count = tokens.shape[0]
    rows, width = query_weight.shape
    heads = gate_weight.shape[1]
    half = width // HALVES
    head_size = width // heads
    wide = rows % 128 == 0
    tok = tokens if wide else tokens.reshape(count, seq, rows).transpose(1, 0, 2)
    gate_t = jnp.pad(gate_weight.T, ((0, 16 - heads), (0, 0)))
    rate = jnp.pad(decay_rate, (0, 8 - heads))[:, None]
    vmem = pl.BlockSpec(memory_space=pltpu.VMEM)
    hbm = pl.BlockSpec(memory_space=pl.ANY)
    pieces = 3 * HALVES + 2
    blocks = count // 256 if count % 256 == 0 else 1
    dma = pltpu.SemaphoreType.DMA
    deep = head_size * heads // HALVES
    out_width = out_weight.shape[1]
    both = (2 * count, tok.shape[1]) if wide else (seq, 2 * count, rows)
    return pl.pallas_call(
        functools.partial(layer_kernel, seq, tp, heads, wide),
        out_shape=jax.ShapeDtypeStruct((count, out_width), jnp.bfloat16),
        in_specs=[hbm, vmem, vmem, hbm, hbm, hbm, hbm, hbm],
        out_specs=vmem,
        scratch_shapes=[
            pltpu.VMEM((seq, 16, rows), jnp.bfloat16),
            pltpu.VMEM((3 * HALVES, seq, rows, half), jnp.bfloat16),
            pltpu.VMEM((2 * count, 16), jnp.float32),
            pltpu.VMEM((3 * HALVES, 2 * count, half), jnp.float32),
            pltpu.VMEM(out_weight.shape, jnp.bfloat16),
            pltpu.VMEM((count, out_width), jnp.float32),
            pltpu.VMEM((2, count, 128), jnp.float32),
            pltpu.VMEM((2, 8, count), jnp.float32),
            pltpu.VMEM((2, HALVES, deep, head_size), jnp.float32),
            pltpu.VMEM((2, HALVES, deep, head_size), jnp.bfloat16),
            pltpu.VMEM((2, HALVES, deep, head_size), jnp.bfloat16),
            pltpu.VMEM((2, HALVES, 8, head_size), jnp.float32),
            pltpu.VMEM((2, HALVES, 8, head_size), jnp.float32),
            pltpu.VMEM((HALVES, deep, head_size), jnp.float32),
            pltpu.VMEM((HALVES, deep, head_size), jnp.float32),
            pltpu.VMEM((2, HALVES, deep, head_size), jnp.bfloat16),
            pltpu.VMEM((HALVES, tp + 1, count, half), jnp.bfloat16),
            pltpu.VMEM(both, jnp.bfloat16),
            dma((pieces + 2,)),
            dma((pieces, 3)),
            dma((pieces, seq)),
            dma((pieces, seq)),
            dma((pieces, seq)),
            dma((PARTS, tp - 1)),
            dma((tp * PARTS,)),
            dma((2, 2, HALVES)),
            dma((2, 2, HALVES)),
            dma((HALVES,)),
            dma((HALVES,)),
            dma((3, blocks, tp - 1)),
            dma((3, blocks, tp)),
            dma((3, blocks)),
        ],
        compiler_params=pltpu.CompilerParams(
            collective_id=0, has_side_effects=True, vmem_limit_bytes=62 * 1024 * 1024
        ),
    )(tok, rate, norm_gain[None, :], gate_t, key_weight, value_weight, query_weight, out_weight)


def solution(mesh):
    return jax.shard_map(
        functools.partial(on_device, mesh.shape["seq"], mesh.shape["tp"]),
        mesh=mesh,
        in_specs=(
            P("seq", None),
            P("seq", "tp"),
            P("seq", "tp"),
            P("seq", "tp"),
            P("seq", "tp"),
            P("tp"),
            P("tp"),
            P(None, "tp"),
        ),
        out_specs=P("seq", "tp"),
        check_vma=False,
    )
```

```python
import functools

import jax
import jax.numpy as jnp
from jax import lax
from jax.experimental import pallas as pl
from jax.experimental.pallas import tpu as pltpu
from jax.sharding import PartitionSpec as P

HALVES = 2
MESH = pl.DeviceIdType.MESH
CROSS = 2
PHASES = [[1, 0], [2], [4], [5], [3], [6], [7]]
EARLY = (2, 3, 5, 6, 7)
PARTS = 8


def layer_kernel(seq, tp, heads, wide, *refs):
    tok_in, rate_ref, gain_ref, gate_in, key_in, value_in, query_in, out_in = refs[:8]
    mixed_ref = refs[8]
    gate_buf, kvq_buf, gate_acc, acc, out_buf, out_acc, wcol, wrow = refs[9:17]
    state_mine, state_wire, state_peer, total_mine, total_peer = refs[17:22]
    state_in, state_next, state_pre, normed_buf, tok_ref = refs[22:27]
    gate_raw = refs[41]
    own_sem, send_own, send_line, send_peer, recv_sem = refs[27:32]
    tok_send, tok_recv, local_send, local_recv, state_send, state_recv = refs[32:38]
    normed_send, normed_recv, guest_send = refs[38:41]
    rows = key_in.shape[0]
    half = key_in.shape[1] // HALVES
    quarter = half // 2
    line = seq // CROSS
    me = lax.axis_index("seq")
    a, b = me // CROSS, me % CROSS
    peer = a * CROSS + (1 - b)
    count = acc.shape[1] // 2
    head_size = 2 * half // heads
    per_half = heads // HALVES
    block = 256 if count % 256 == 0 else count
    blocks = count // block
    col = lax.axis_index("tp")
    pair_col = col + 1 - 2 * (col % 2)
    groups = tp // 2
    last = line - 1
    is_end = (a == 0) | (a == last)
    is_worker = (a > 0) & (a < last)
    all_hosts = line == 4
    is_host = (a == 1) | (a == last - 1)
    is_low = a == 1
    up_works, down_works = a + 1 < last, a - 1 > 0
    partner = jnp.where((a == 0) | ((a == last - 1) & (a != 1)), me + CROSS, me - CROSS)
    units = [
        (0, 0, half, range(per_half)),
        (1, 0, quarter, range(per_half // 2)),
        (1, quarter, quarter, range(per_half // 2, per_half)),
    ]

    def hosts(run):
        if all_hosts:
            run()
        else:
            pl.when(is_host)(run)

    def buffer(piece, source):
        if piece == 0:
            return gate_buf.at[source]
        if piece >= 3 * HALVES:
            at = pl.ds((piece - 3 * HALVES) * quarter, quarter)
            return kvq_buf.at[3 * HALVES - 1, source, :, at]
        return kvq_buf.at[piece - 1, source]

    def copy(piece, source, sem, target):
        return pltpu.make_async_remote_copy(
            src_ref=buffer(piece, source),
            dst_ref=buffer(piece, source),
            send_sem=sem,
            recv_sem=recv_sem.at[piece, source],
            device_id={"seq": target},
            device_id_type=MESH,
        )

    def arrive(piece, source):
        copy(piece, source, send_own.at[piece, 0], peer).wait_recv()

    loads = [pltpu.make_async_copy(gate_in, gate_raw, own_sem.at[0])]
    for index in range(3 * HALVES):
        source_ref = (key_in, value_in, query_in)[index % 3]
        at = (index // 3) * half
        loads.append(
            pltpu.make_async_copy(
                source_ref.at[:, pl.ds(at, half)], kvq_buf.at[index, me], own_sem.at[index + 1]
            )
        )
    for load in loads:
        load.start()
    if wide:
        own_tok = tok_ref.at[pl.ds(0, count), :]
    else:
        own_tok = tok_ref.at[:, pl.ds(0, count), :]
    tok_load = pltpu.make_async_copy(tok_in, own_tok, own_sem.at[3 * HALVES + 2])
    pl.when(is_worker)(tok_load.start)
    out_load = pltpu.make_async_copy(out_in, out_buf, own_sem.at[3 * HALVES + 1])
    out_load.start()

    barrier = pltpu.get_barrier_semaphore()
    has_up, has_down = a < last, a > 0
    pl.semaphore_signal(barrier, inc=1, device_id={"seq": peer}, device_id_type=MESH)

    @pl.when(has_up)
    def _():
        pl.semaphore_signal(barrier, inc=1, device_id={"seq": me + CROSS}, device_id_type=MESH)

    @pl.when(has_down)
    def _():
        pl.semaphore_signal(barrier, inc=1, device_id={"seq": me - CROSS}, device_id_type=MESH)

    pl.semaphore_signal(barrier, inc=1, device_id={"tp": pair_col}, device_id_type=MESH)
    for g in range(1, groups):
        pl.semaphore_signal(
            barrier, inc=1, device_id={"tp": lax.rem(col + 2 * g, tp)}, device_id_type=MESH
        )
    pl.semaphore_wait(barrier, 1 + groups + has_up.astype(jnp.int32) + has_down.astype(jnp.int32))

    def load_wait(piece):
        if piece <= 3 * HALVES:
            loads[piece].wait()
        if piece == 0:
            raw = gate_raw[...].astype(jnp.float32)
            raw = jnp.concatenate([raw, jnp.zeros((rows, 128 - heads), jnp.float32)], axis=1)
            gate_buf[me] = raw.T[:16].astype(jnp.bfloat16)

    def ready(number):
        for piece in PHASES[number]:
            load_wait(piece)

    def far(g):
        return lax.rem(col + 2 * g, tp)

    def far_pair(g):
        return lax.rem(pair_col + 2 * g, tp)

    def own_line(number):
        for piece in PHASES[number]:

            @pl.when(up_works)
            def _():
                copy(piece, me, send_own.at[piece, 1], me + CROSS).start()

            @pl.when(down_works)
            def _():
                copy(piece, me, send_own.at[piece, 2], me - CROSS).start()

    def own_cross(number):
        for piece in PHASES[number]:
            copy(piece, me, send_own.at[piece, 0], peer).start()

    def each_middle(run):
        @pl.loop(0, 2 * (line - 3))
        def _(n):
            sign = 1 - 2 * (n % 2)
            origin = a - sign * (1 + n // 2)
            onward = (a + sign > 0) & (a + sign < last)

            @pl.when((origin > 0) & (origin < last))
            def _():
                run(origin, onward, me + sign * CROSS)

    near_low = 2 * a < line
    near_origin = jnp.where(near_low, 0, last)
    far_origin = last - near_origin
    near_onward = jnp.where(near_low, up_works, down_works)
    far_onward = jnp.where(near_low, down_works, up_works)
    away = jnp.where(near_low, CROSS, -CROSS)

    def ends():
        return (near_origin, near_onward, me + away), (far_origin, far_onward, me - away)

    def middle(number):
        def run(origin, onward, target):
            source = origin * CROSS + b
            for piece in PHASES[number]:
                arrive(piece, source)
                copy(piece, source, send_peer.at[piece, source], peer).start()

                @pl.when(onward)
                def _():
                    copy(piece, source, send_line.at[piece, source], target).start()

        each_middle(run)

    def outer(number, which, side):
        origin, onward, target = ends()[which]
        source = origin * CROSS + (b if side == 0 else 1 - b)
        for piece in PHASES[number]:
            arrive(piece, source)

            @pl.when(onward)
            def _():
                copy(piece, source, send_line.at[piece, source], target).start()

            if piece not in EARLY:
                copy(piece, source, send_peer.at[piece, source], peer).start()

    def tok_part(ref, index, base):
        if wide:
            size = ref.shape[1] // (tp * PARTS)
            at = pl.ds(pl.multiple_of(index * size, size), size)
            return ref.at[pl.ds(base, count), at]
        size = seq // (tp * PARTS)
        return ref.at[pl.ds(index * size, size), pl.ds(base, count), :]

    def tok_copy(index, j, send, target, first=False):
        return pltpu.make_async_remote_copy(
            src_ref=tok_part(tok_in, index, 0) if first else tok_part(tok_ref, index, count),
            dst_ref=tok_part(tok_ref, index, count),
            send_sem=tok_send.at[j, send],
            recv_sem=tok_recv.at[index],
            device_id=target,
            device_id_type=MESH,
        )

    def tok_arrive(index):
        tok_copy(index, 0, 0, {"tp": pair_col}).wait_recv()

    def tok_spread(j):
        def run():
            index = col * PARTS + j
            tok_arrive(index)
            for g in range(1, groups):
                tok_copy(index, j, g, {"tp": far(g)}).start()
            tok_copy(index, j, 0, {"tp": pair_col}).start()

        hosts(run)

    def tok_relay(j):
        def run():
            for g in range(1, groups):
                index = far(g) * PARTS + j
                tok_arrive(index)
                tok_copy(index, j, groups - 1 + g, {"tp": pair_col}).start()

        hosts(run)

    def tok_rest():
        def run():
            for j in range(PARTS):
                tok_arrive(pair_col * PARTS + j)
                for g in range(1, groups):
                    tok_arrive(far_pair(g) * PARTS + j)

        hosts(run)

    def multiply(piece, source, base, size):
        at = slice(base, base + size)
        if wide:
            x = tok_ref[at, pl.ds(pl.multiple_of(source * rows, rows), rows)]
        else:
            x = tok_ref[source, at]
        if piece == 0:
            gate_acc[at] += lax.dot_general(
                x, gate_buf[source], (((1,), (1,)), ((), ())), preferred_element_type=jnp.float32
            )
        elif piece >= 3 * HALVES:
            cols = slice((piece - 3 * HALVES) * quarter, (piece - 3 * HALVES + 1) * quarter)
            acc[3 * HALVES - 1, at, cols] += jnp.dot(
                x, kvq_buf[3 * HALVES - 1, source, :, cols], preferred_element_type=jnp.float32
            )
        else:
            acc[piece - 1, at] += jnp.dot(
                x, kvq_buf[piece - 1, source], preferred_element_type=jnp.float32
            )

    def product(piece, source, part):
        if part == "own":
            multiply(piece, source, 0, count)
        elif part == "guest":
            hosts(lambda: multiply(piece, source, count, count))
        elif all_hosts:
            multiply(piece, source, 0, 2 * count)
        else:

            @pl.when(is_host)
            def _():
                multiply(piece, source, 0, 2 * count)

            @pl.when(jnp.logical_not(is_host))
            def _():
                multiply(piece, source, 0, count)

    def mine(number, part):
        for piece in PHASES[number]:
            product(piece, me, part)

    def middles(number, part):
        def run(origin, onward, target):
            for piece in PHASES[number]:
                product(piece, origin * CROSS + b, part)

        each_middle(run)

    def outside(number, which, part):
        origin = ends()[which][0]
        for piece in PHASES[number]:
            if piece in EARLY:

                @pl.loop(0, CROSS)
                def _(side):
                    product(piece, origin * CROSS + side, part)

            else:
                product(piece, origin * CROSS + b, part)

    def crossed_mine(number, part):
        for piece in PHASES[number]:
            arrive(piece, peer)
            product(piece, peer, part)

    def crossed(number, part):
        pieces = PHASES[number]

        def run(origin, onward, target):
            for piece in pieces:
                source = origin * CROSS + (1 - b)
                arrive(piece, source)
                product(piece, source, part)

        each_middle(run)

    def crossed_outside(number, which, part):
        for piece in PHASES[number]:
            if piece not in EARLY:
                source = ends()[which][0] * CROSS + (1 - b)
                arrive(piece, source)
                product(piece, source, part)

    def guests(number, rest=True):
        pieces = PHASES[number]

        def run():
            if rest:

                @pl.loop(0, seq)
                def _(source):
                    for piece in pieces:
                        multiply(piece, source, count, count)

            else:

                @pl.loop(CROSS, seq - CROSS)
                def _(source):
                    for piece in pieces:
                        multiply(piece, source, count, count)

        hosts(run)

    trips = 2 if all_hosts else 1 + is_host.astype(jnp.int32)
    first_group = jnp.where(is_low, 1, 0)
    second_group = 1 - first_group

    def token_rows(w, start, size):
        return pl.ds(pl.multiple_of(w * count + start, block), size)

    def decays():
        @pl.loop(0, trips)
        def _(w):
            logits = jnp.concatenate(
                [
                    gate_acc[token_rows(w, 0, count)],
                    jnp.zeros((count, 128 - gate_acc.shape[1]), jnp.float32),
                ],
                axis=1,
            ).T[:8]
            soft = jnp.maximum(logits, 0.0) + jnp.log1p(jnp.exp(-jnp.abs(logits)))
            head_row = lax.broadcasted_iota(jnp.int32, soft.shape, 0)
            rate = jnp.zeros(soft.shape, jnp.float32)
            for head in range(heads):
                rate = jnp.where(head_row == head, rate_ref[head], rate)
            total = -rate * soft
            lane = lax.broadcasted_iota(jnp.int32, total.shape, 1)
            reach = 1
            while reach < count:
                total = total + jnp.where(lane >= reach, pltpu.roll(total, reach, 1), 0.0)
                reach *= 2
            wrow[w] = total
            wcol[w] = jnp.concatenate([total, jnp.zeros((120, count), jnp.float32)], axis=0).T

    class local_copy:
        def __init__(self, h, slot, group):
            pairs = ((state_wire, state_peer), (total_mine, total_peer))
            self.copies = [
                pltpu.make_async_remote_copy(
                    src_ref=source.at[group, h],
                    dst_ref=target.at[slot, h],
                    send_sem=local_send.at[n, slot, h],
                    recv_sem=local_recv.at[n, slot, h],
                    device_id={"seq": peer},
                    device_id_type=MESH,
                )
                for n, (source, target) in enumerate(pairs)
            ]

        def start(self):
            for one in self.copies:
                one.start()

        def wait_recv(self):
            for one in self.copies:
                one.wait_recv()

        def wait_send(self):
            for one in self.copies:
                one.wait_send()

    def local_state(h):
        @pl.loop(0, trips)
        def _(w):
            for j in range(per_half):
                head = h * per_half + j
                cols = slice(j * head_size, (j + 1) * head_size)
                within = wcol[w, :, head : head + 1]
                final = wcol[w, count - 1 : count, head : head + 1]
                at = token_rows(w, 0, count)
                key = acc[3 * h, at, cols].astype(jnp.bfloat16).astype(jnp.float32)
                scaled = (jnp.exp(final - within) * key).astype(jnp.bfloat16)
                value = acc[3 * h + 1, at, cols].astype(jnp.bfloat16)
                local = lax.dot_general(
                    scaled, value, (((0,), (0,)), ((), ())), preferred_element_type=jnp.float32
                )
                state_mine[w, h, j * head_size : (j + 1) * head_size] = local
                state_wire[w, h, j * head_size : (j + 1) * head_size] = local.astype(jnp.bfloat16)
                total_mine[w, h, j : j + 1] = jnp.broadcast_to(final, (1, head_size))

        local_copy(h, 0, first_group).start()
        hosts(lambda: local_copy(h, 1, second_group).start())

    def line_state(h):
        return pltpu.make_async_remote_copy(
            src_ref=state_next.at[h],
            dst_ref=state_in.at[h],
            send_sem=state_send.at[h],
            recv_sem=state_recv.at[h],
            device_id={"seq": me + CROSS},
            device_id_type=MESH,
        )

    def chain(h):
        @pl.when(is_low)
        def _():
            state_in[h] = jnp.zeros(state_in.shape[1:], jnp.float32)

        @pl.when(jnp.logical_not(is_low))
        def _():
            line_state(h).wait_recv()

        spans = [slice(j * head_size, (j + 1) * head_size) for j in range(per_half)]

        def step(state, j, slot, group, peers):
            own = (total_mine[group, h, j : j + 1], state_mine[group, h, spans[j]])
            other = (
                total_peer[slot, h, j : j + 1],
                state_peer[slot, h, spans[j]].astype(jnp.float32),
            )
            total = jnp.where(peers, other[0], own[0])
            return jnp.exp(total) * state + jnp.where(peers, other[1], own[1])

        def pass_group(slot, group):
            local_copy(h, slot, group).wait_recv()
            for j, at in enumerate(spans):
                state = state_in[h, at] if slot == 0 else state_next[h, at]
                middle_state = step(state, j, slot, group, b == 1)
                state_pre[group, h, at] = jnp.where(b == 1, middle_state, state).astype(
                    jnp.bfloat16
                )
                state_next[h, at] = step(middle_state, j, slot, group, b == 0)

        pass_group(0, first_group)
        hosts(lambda: pass_group(1, second_group))

        @pl.when(up_works)
        def _():
            line_state(h).start()

    def block_rows(i):
        return pl.ds(i * block if isinstance(i, int) else pl.multiple_of(i * block, block), block)

    def normed_copy(u, i, source, send, target):
        h, start, size, _ = units[u]
        ref = normed_buf.at[h, source, block_rows(i), pl.ds(start, size)]
        return pltpu.make_async_remote_copy(
            src_ref=ref,
            dst_ref=ref,
            send_sem=normed_send.at[u, i, send],
            recv_sem=normed_recv.at[u, i, source],
            device_id={"tp": target},
            device_id_type=MESH,
        )

    def guest_copy(u, i):
        h, start, size, _ = units[u]
        return pltpu.make_async_remote_copy(
            src_ref=normed_buf.at[h, tp, block_rows(i), pl.ds(start, size)],
            dst_ref=normed_buf.at[h, col, block_rows(i), pl.ds(start, size)],
            send_sem=guest_send.at[u, i],
            recv_sem=normed_recv.at[u, i, col],
            device_id={"seq": partner},
            device_id_type=MESH,
        )

    def share(u, i):
        for g in range(1, groups):
            normed_copy(u, i, col, g, far(g)).start()
        normed_copy(u, i, col, 0, pair_col).start()

    def relay(u, i):
        for g in range(1, groups):
            normed_copy(u, i, far(g), 0, pair_col).wait_recv()
            normed_copy(u, i, far(g), groups - 1 + g, pair_col).start()

    def attention(u):
        h, _, _, members = units[u]

        @pl.loop(0, trips)
        def _(n):
            w = trips - 1 - n
            slot = jnp.where(w == 0, col, tp)
            for i in range(blocks):
                upto = (i + 1) * block
                row = i * block + lax.broadcasted_iota(jnp.int32, (block, upto), 0)
                causal = lax.broadcasted_iota(jnp.int32, (block, upto), 1) <= row
                t_at = token_rows(w, i * block, block)
                s_at = token_rows(w, 0, upto)
                for j in members:
                    head = h * per_half + j
                    cols = slice(j * head_size, (j + 1) * head_size)
                    query = acc[3 * h + 2, t_at, cols].astype(jnp.bfloat16)
                    key = acc[3 * h, s_at, cols].astype(jnp.bfloat16)
                    value = acc[3 * h + 1, s_at, cols].astype(jnp.bfloat16)
                    within = wcol[w, i * block : (i + 1) * block, head : head + 1]
                    scores = lax.dot_general(
                        query, key, (((1,), (1,)), ((), ())), preferred_element_type=jnp.float32
                    )
                    gap = within - wrow[w, head : head + 1, :upto]
                    attn = jnp.where(causal, scores * jnp.exp(jnp.where(causal, gap, 0.0)), 0.0)
                    local = jnp.dot(
                        attn.astype(jnp.bfloat16), value, preferred_element_type=jnp.float32
                    )
                    scaled = (jnp.exp(within) * query.astype(jnp.float32)).astype(jnp.bfloat16)
                    state = state_pre[w, h, j * head_size : (j + 1) * head_size]
                    head_out = local + jnp.dot(scaled, state, preferred_element_type=jnp.float32)
                    square = jnp.mean(head_out * head_out, axis=-1, keepdims=True)
                    gain = gain_ref[:, head * head_size : (head + 1) * head_size]
                    normed_buf[h, slot, i * block : (i + 1) * block, cols] = (
                        head_out * lax.rsqrt(square + 1e-05) * gain
                    ).astype(jnp.bfloat16)

                @pl.when(w == 0)
                def _():
                    share(u, i)

                @pl.when(w == 1)
                def _():
                    guest_copy(u, i).start()

    def settle(h):
        mine = [u for u in range(len(units)) if units[u][0] == h]

        def mix(i, source):
            depth = pl.ds(pl.multiple_of((source * HALVES + h) * half, half), half)
            return jnp.dot(
                normed_buf[h, source, block_rows(i)],
                out_buf[depth, :],
                preferred_element_type=jnp.float32,
            )

        @pl.loop(0, blocks)
        def _(i):
            at = block_rows(i)
            total = mix(i, col)
            for u in mine:
                normed_copy(u, i, pair_col, 0, pair_col).wait_recv()
            total = total + mix(i, pair_col)
            for g in range(1, groups):
                total = total + mix(i, far(g))
                for u in mine:
                    normed_copy(u, i, far_pair(g), 0, pair_col).wait_recv()
                total = total + mix(i, far_pair(g))
            if h == 0:
                out_acc[at, :] = total
            else:
                mixed_ref[at, :] = (out_acc[at, :] + total).astype(jnp.bfloat16)

    def relays(u):
        @pl.loop(0, blocks)
        def _(i):
            relay(u, i)

    @pl.when(is_end)
    def _():
        for j in range(PARTS):
            tok_copy(col * PARTS + j, j, 0, {"seq": partner}, True).start()
        for pieces in PHASES:
            for piece in pieces:
                load_wait(piece)
                if piece in EARLY:
                    copy(piece, me, send_own.at[piece, 0], peer).start()
        for pieces in PHASES:
            for piece in pieces:
                copy(piece, me, send_own.at[piece, 1], partner).start()
                if piece in EARLY:
                    arrive(piece, peer)
                    copy(piece, peer, send_line.at[piece, peer], partner).start()
        out_load.wait()

        def hand_out(u):
            @pl.loop(0, blocks)
            def _(i):
                guest_copy(u, i).wait_recv()
                share(u, i)

        hand_out(0)
        hand_out(1)
        relays(0)
        hand_out(2)
        relays(1)
        settle(0)
        relays(2)

    @pl.when(is_worker)
    def _():
        gate_acc[...] = jnp.zeros_like(gate_acc)
        acc[...] = jnp.zeros_like(acc)
        ready(0)
        own_cross(0)
        own_line(0)
        tok_spread(0)
        ready(1)
        own_cross(1)
        own_line(1)
        tok_spread(1)
        middle(0)
        tok_relay(0)
        middle(1)
        tok_spread(2)
        ready(2)
        own_line(2)
        tok_spread(3)
        own_cross(2)
        tok_spread(4)
        ready(4)
        tok_load.wait()
        mine(4, "own")
        ready(3)
        own_cross(3)
        own_line(3)
        crossed_mine(1, "own")
        tok_relay(1)
        own_line(4)
        middle(2)
        tok_relay(2)
        ready(5)
        own_line(5)
        tok_spread(5)
        crossed(0, "own")
        middles(0, "own")
        ready(6)
        own_line(6)
        tok_relay(3)
        middle(3)
        tok_spread(6)
        outer(0, 0, 0)
        mine(5, "own")
        tok_spread(7)
        crossed_mine(2, "own")
        tok_relay(4)
        tok_relay(5)
        mine(1, "own")
        outer(1, 0, 0)
        crossed(1, "own")
        tok_relay(6)
        mine(6, "own")
        tok_relay(7)
        outer(0, 1, 0)
        own_cross(4)
        middles(3, "own")
        middles(2, "own")
        mine(3, "own")
        crossed(3, "own")
        crossed_mine(0, "own")
        tok_rest()
        outer(1, 0, 1)
        outside(1, 0, "both")
        guests(1, False)
        crossed_mine(3, "own")
        outside(0, 1, "own")
        crossed_outside(0, 0, "own")
        outer(2, 0, 0)
        guests(3, False)
        outside(0, 0, "own")
        mine(2, "own")
        outer(1, 1, 1)
        crossed_outside(0, 1, "own")
        outer(1, 1, 0)
        outside(1, 1, "both")
        outer(3, 0, 0)
        guests(0)
        outside(2, 0, "own")
        middles(1, "own")
        mine(0, "own")
        crossed(2, "own")
        outer(2, 1, 0)
        outside(2, 1, "own")
        outer(3, 0, 1)
        decays()
        middle(4)
        crossed_mine(4, "own")
        middles(4, "own")
        local_state(0)
        middle(5)
        crossed_outside(2, 0, "own")
        outer(3, 1, 0)
        middles(5, "own")
        outer(4, 0, 0)
        middle(6)
        outside(3, 0, "both")
        crossed_outside(2, 1, "own")
        guests(2)
        outer(4, 0, 1)
        outside(4, 0, "both")
        outer(3, 1, 1)
        crossed(4, "own")
        outside(3, 1, "both")
        local_state(1)
        outer(4, 1, 0)
        middles(6, "own")
        own_cross(5)
        chain(0)
        guests(4, False)
        own_cross(6)
        outer(5, 0, 0)
        outer(5, 0, 1)
        outer(4, 1, 1)
        outside(4, 1, "both")
        attention(0)
        outside(5, 0, "both")
        chain(1)
        outer(6, 0, 0)
        crossed_mine(5, "own")
        outer(6, 0, 1)
        outside(6, 0, "both")
        crossed_mine(6, "own")
        outer(5, 1, 1)
        outer(5, 1, 0)
        outside(5, 1, "both")
        crossed(5, "own")
        guests(5, False)
        attention(1)
        crossed(6, "own")
        guests(6, False)
        outer(6, 1, 1)
        outer(6, 1, 0)
        outside(6, 1, "both")
        attention(2)
        relays(0)
        relays(1)
        out_load.wait()
        settle(0)
        relays(2)

    settle(1)

    @pl.loop(0, blocks)
    def _(i):
        for u in range(len(units)):
            for k in range(tp - 1):
                normed_copy(u, i, col, k, pair_col).wait_send()

    @pl.when(is_end)
    def _():
        for pieces in PHASES:
            for piece in pieces:
                copy(piece, me, send_own.at[piece, 1], peer).wait_send()
                if piece in EARLY:
                    copy(piece, me, send_own.at[piece, 0], peer).wait_send()
                    copy(piece, peer, send_line.at[piece, peer], peer).wait_send()
        for j in range(PARTS):
            tok_copy(col * PARTS + j, j, 0, {"seq": partner}, True).wait_send()

    @pl.when(is_worker)
    def _():
        def host_drain():
            for j in range(PARTS):
                for k in range(tp - 1):
                    tok_copy(col * PARTS + j, j, k, {"tp": pair_col}).wait_send()

            @pl.loop(0, blocks)
            def _(i):
                for u in range(len(units)):
                    guest_copy(u, i).wait_send()

        hosts(host_drain)
        for h in range(HALVES):

            local_copy(h, 0, first_group).wait_send()
            hosts(lambda: local_copy(h, 1, second_group).wait_send())

            @pl.when(up_works)
            def _():
                line_state(h).wait_send()

        for pieces in PHASES:
            for piece in pieces:
                copy(piece, me, send_own.at[piece, 0], peer).wait_send()

                @pl.when(up_works)
                def _():
                    copy(piece, me, send_own.at[piece, 1], peer).wait_send()

                @pl.when(down_works)
                def _():
                    copy(piece, me, send_own.at[piece, 2], peer).wait_send()

                for origin, onward, _ in ends():
                    source, other = origin * CROSS + b, origin * CROSS + (1 - b)

                    @pl.when(onward)
                    def _():
                        copy(piece, source, send_line.at[piece, source], peer).wait_send()
                        if piece in EARLY:
                            copy(piece, other, send_line.at[piece, other], peer).wait_send()

                    if piece not in EARLY:
                        copy(piece, source, send_peer.at[piece, source], peer).wait_send()

        def run(origin, onward, target):
            source = origin * CROSS + b
            for pieces in PHASES:
                for piece in pieces:
                    copy(piece, source, send_peer.at[piece, source], peer).wait_send()

                    @pl.when(onward)
                    def _():
                        copy(piece, source, send_line.at[piece, source], peer).wait_send()

        each_middle(run)


def on_device(
    seq,
    tp,
    tokens,
    query_weight,
    key_weight,
    value_weight,
    gate_weight,
    decay_rate,
    norm_gain,
    out_weight,
):
    count = tokens.shape[0]
    rows, width = query_weight.shape
    heads = gate_weight.shape[1]
    half = width // HALVES
    head_size = width // heads
    wide = rows % 128 == 0
    tok = tokens if wide else tokens.reshape(count, seq, rows).transpose(1, 0, 2)
    vmem = pl.BlockSpec(memory_space=pltpu.VMEM)
    smem = pl.BlockSpec(memory_space=pltpu.SMEM)
    hbm = pl.BlockSpec(memory_space=pl.ANY)
    pieces = 3 * HALVES + 2
    blocks = count // 256 if count % 256 == 0 else 1
    dma = pltpu.SemaphoreType.DMA
    deep = head_size * heads // HALVES
    out_width = out_weight.shape[1]
    both = (2 * count, tok.shape[1]) if wide else (seq, 2 * count, rows)
    return pl.pallas_call(
        functools.partial(layer_kernel, seq, tp, heads, wide),
        out_shape=jax.ShapeDtypeStruct((count, out_width), jnp.bfloat16),
        in_specs=[hbm, smem, vmem, hbm, hbm, hbm, hbm, hbm],
        out_specs=vmem,
        scratch_shapes=[
            pltpu.VMEM((seq, 16, rows), jnp.bfloat16),
            pltpu.VMEM((3 * HALVES, seq, rows, half), jnp.bfloat16),
            pltpu.VMEM((2 * count, 16), jnp.float32),
            pltpu.VMEM((3 * HALVES, 2 * count, half), jnp.float32),
            pltpu.VMEM(out_weight.shape, jnp.bfloat16),
            pltpu.VMEM((count, out_width), jnp.float32),
            pltpu.VMEM((2, count, 128), jnp.float32),
            pltpu.VMEM((2, 8, count), jnp.float32),
            pltpu.VMEM((2, HALVES, deep, head_size), jnp.float32),
            pltpu.VMEM((2, HALVES, deep, head_size), jnp.bfloat16),
            pltpu.VMEM((2, HALVES, deep, head_size), jnp.bfloat16),
            pltpu.VMEM((2, HALVES, 8, head_size), jnp.float32),
            pltpu.VMEM((2, HALVES, 8, head_size), jnp.float32),
            pltpu.VMEM((HALVES, deep, head_size), jnp.float32),
            pltpu.VMEM((HALVES, deep, head_size), jnp.float32),
            pltpu.VMEM((2, HALVES, deep, head_size), jnp.bfloat16),
            pltpu.VMEM((HALVES, tp + 1, count, half), jnp.bfloat16),
            pltpu.VMEM(both, jnp.bfloat16),
            dma((pieces + 2,)),
            dma((pieces, 3)),
            dma((pieces, seq)),
            dma((pieces, seq)),
            dma((pieces, seq)),
            dma((PARTS, tp - 1)),
            dma((tp * PARTS,)),
            dma((2, 2, HALVES)),
            dma((2, 2, HALVES)),
            dma((HALVES,)),
            dma((HALVES,)),
            dma((3, blocks, tp - 1)),
            dma((3, blocks, tp)),
            dma((3, blocks)),
            pltpu.VMEM((rows, heads), jnp.bfloat16),
        ],
        compiler_params=pltpu.CompilerParams(
            collective_id=0, has_side_effects=True, vmem_limit_bytes=62 * 1024 * 1024
        ),
    )(tok, decay_rate, norm_gain[None, :], gate_weight, key_weight, value_weight, query_weight, out_weight)


def solution(mesh):
    return jax.shard_map(
        functools.partial(on_device, mesh.shape["seq"], mesh.shape["tp"]),
        mesh=mesh,
        in_specs=(
            P("seq", None),
            P("seq", "tp"),
            P("seq", "tp"),
            P("seq", "tp"),
            P("seq", "tp"),
            P("tp"),
            P("tp"),
            P(None, "tp"),
        ),
        out_specs=P("seq", "tp"),
        check_vma=False,
    )
```

```python
import functools

import jax
import jax.numpy as jnp
from jax import lax
from jax.experimental import pallas as pl
from jax.experimental.pallas import tpu as pltpu
from jax.sharding import PartitionSpec as P

HALVES = 2
MESH = pl.DeviceIdType.MESH
CROSS = 2
PHASES = [[1, 0], [2], [4], [5], [3], [6], [7]]
EARLY = (2, 3, 5, 6, 7)
PARTS = 8


def layer_kernel(seq, tp, heads, wide, *refs):
    tok_in, rate_ref, gain_ref, gate_in, key_in, value_in, query_in, out_in = refs[:8]
    mixed_ref = refs[8]
    gate_buf, kvq_buf, gate_acc, acc, out_buf, out_acc, wcol, wrow = refs[9:17]
    state_mine, state_wire, state_peer, total_mine, total_peer = refs[17:22]
    state_in, state_next, state_pre, normed_buf, tok_ref = refs[22:27]
    gate_raw = refs[41]
    own_sem, send_own, send_line, send_peer, recv_sem = refs[27:32]
    tok_send, tok_recv, local_send, local_recv, state_send, state_recv = refs[32:38]
    normed_send, normed_recv, guest_send = refs[38:41]
    rows = key_in.shape[0]
    half = key_in.shape[1] // HALVES
    quarter = half // 2
    line = seq // CROSS
    me = lax.axis_index("seq")
    a, b = me // CROSS, me % CROSS
    peer = a * CROSS + (1 - b)
    count = acc.shape[1] // 2
    head_size = 2 * half // heads
    per_half = heads // HALVES
    block = 256 if count % 256 == 0 else count
    blocks = count // block
    col = lax.axis_index("tp")
    pair_col = col + 1 - 2 * (col % 2)
    groups = tp // 2
    last = line - 1
    is_end = (a == 0) | (a == last)
    is_worker = (a > 0) & (a < last)
    all_hosts = line == 4
    is_host = (a == 1) | (a == last - 1)
    is_low = a == 1
    up_works, down_works = a + 1 < last, a - 1 > 0
    partner = jnp.where((a == 0) | ((a == last - 1) & (a != 1)), me + CROSS, me - CROSS)
    units = [
        (0, 0, half, range(per_half)),
        (1, 0, quarter, range(per_half // 2)),
        (1, quarter, quarter, range(per_half // 2, per_half)),
    ]

    def hosts(run):
        if all_hosts:
            run()
        else:
            pl.when(is_host)(run)

    def buffer(piece, source):
        if piece == 0:
            return gate_buf.at[source]
        if piece >= 3 * HALVES:
            at = pl.ds((piece - 3 * HALVES) * quarter, quarter)
            return kvq_buf.at[3 * HALVES - 1, source, :, at]
        return kvq_buf.at[piece - 1, source]

    def copy(piece, source, sem, target):
        return pltpu.make_async_remote_copy(
            src_ref=buffer(piece, source),
            dst_ref=buffer(piece, source),
            send_sem=sem,
            recv_sem=recv_sem.at[piece, source],
            device_id={"seq": target},
            device_id_type=MESH,
        )

    def arrive(piece, source):
        copy(piece, source, send_own.at[piece, 0], peer).wait_recv()

    loads = [pltpu.make_async_copy(gate_in, gate_raw, own_sem.at[0])]
    for index in range(3 * HALVES):
        source_ref = (key_in, value_in, query_in)[index % 3]
        at = (index // 3) * half
        loads.append(
            pltpu.make_async_copy(
                source_ref.at[:, pl.ds(at, half)], kvq_buf.at[index, me], own_sem.at[index + 1]
            )
        )
    for load in loads:
        load.start()
    if wide:
        own_tok = tok_ref.at[pl.ds(0, count), :]
    else:
        own_tok = tok_ref.at[:, pl.ds(0, count), :]
    tok_load = pltpu.make_async_copy(tok_in, own_tok, own_sem.at[3 * HALVES + 2])
    pl.when(is_worker)(tok_load.start)
    out_load = pltpu.make_async_copy(out_in, out_buf, own_sem.at[3 * HALVES + 1])
    out_load.start()

    barrier = pltpu.get_barrier_semaphore()
    has_up, has_down = a < last, a > 0
    pl.semaphore_signal(barrier, inc=1, device_id={"seq": peer}, device_id_type=MESH)

    @pl.when(has_up)
    def _():
        pl.semaphore_signal(barrier, inc=1, device_id={"seq": me + CROSS}, device_id_type=MESH)

    @pl.when(has_down)
    def _():
        pl.semaphore_signal(barrier, inc=1, device_id={"seq": me - CROSS}, device_id_type=MESH)

    pl.semaphore_signal(barrier, inc=1, device_id={"tp": pair_col}, device_id_type=MESH)
    for g in range(1, groups):
        pl.semaphore_signal(
            barrier, inc=1, device_id={"tp": lax.rem(col + 2 * g, tp)}, device_id_type=MESH
        )
    pl.semaphore_wait(barrier, 1 + groups + has_up.astype(jnp.int32) + has_down.astype(jnp.int32))

    def load_wait(piece):
        if piece <= 3 * HALVES:
            loads[piece].wait()
        if piece == 0:
            raw = gate_raw[...].astype(jnp.float32)
            raw = jnp.concatenate([raw, jnp.zeros((rows, 128 - heads), jnp.float32)], axis=1)
            gate_buf[me] = raw.T[:16].astype(jnp.bfloat16)

    def ready(number):
        for piece in PHASES[number]:
            load_wait(piece)

    def far(g):
        return lax.rem(col + 2 * g, tp)

    def far_pair(g):
        return lax.rem(pair_col + 2 * g, tp)

    def own_line(number):
        for piece in PHASES[number]:

            @pl.when(up_works)
            def _():
                copy(piece, me, send_own.at[piece, 1], me + CROSS).start()

            @pl.when(down_works)
            def _():
                copy(piece, me, send_own.at[piece, 2], me - CROSS).start()

    def own_cross(number):
        for piece in PHASES[number]:
            copy(piece, me, send_own.at[piece, 0], peer).start()

    def each_middle(run):
        @pl.loop(0, 2 * (line - 3))
        def _(n):
            sign = 1 - 2 * (n % 2)
            origin = a - sign * (1 + n // 2)
            onward = (a + sign > 0) & (a + sign < last)

            @pl.when((origin > 0) & (origin < last))
            def _():
                run(origin, onward, me + sign * CROSS)

    near_low = 2 * a < line
    near_origin = jnp.where(near_low, 0, last)
    far_origin = last - near_origin
    near_onward = jnp.where(near_low, up_works, down_works)
    far_onward = jnp.where(near_low, down_works, up_works)
    away = jnp.where(near_low, CROSS, -CROSS)

    def ends():
        return (near_origin, near_onward, me + away), (far_origin, far_onward, me - away)

    def middle(number):
        def run(origin, onward, target):
            source = origin * CROSS + b
            for piece in PHASES[number]:
                arrive(piece, source)
                copy(piece, source, send_peer.at[piece, source], peer).start()

                @pl.when(onward)
                def _():
                    copy(piece, source, send_line.at[piece, source], target).start()

        each_middle(run)

    def outer(number, which, side):
        origin, onward, target = ends()[which]
        source = origin * CROSS + (b if side == 0 else 1 - b)
        for piece in PHASES[number]:
            arrive(piece, source)

            @pl.when(onward)
            def _():
                copy(piece, source, send_line.at[piece, source], target).start()

            if piece not in EARLY:
                copy(piece, source, send_peer.at[piece, source], peer).start()

    def tok_part(ref, index, base):
        if wide:
            size = ref.shape[1] // (tp * PARTS)
            at = pl.ds(pl.multiple_of(index * size, size), size)
            return ref.at[pl.ds(base, count), at]
        size = seq // (tp * PARTS)
        return ref.at[pl.ds(index * size, size), pl.ds(base, count), :]

    def tok_copy(index, j, send, target, first=False):
        return pltpu.make_async_remote_copy(
            src_ref=tok_part(tok_in, index, 0) if first else tok_part(tok_ref, index, count),
            dst_ref=tok_part(tok_ref, index, count),
            send_sem=tok_send.at[j, send],
            recv_sem=tok_recv.at[index],
            device_id=target,
            device_id_type=MESH,
        )

    def tok_arrive(index):
        tok_copy(index, 0, 0, {"tp": pair_col}).wait_recv()

    def tok_spread(j):
        def run():
            index = col * PARTS + j
            tok_arrive(index)
            for g in range(1, groups):
                tok_copy(index, j, g, {"tp": far(g)}).start()
            tok_copy(index, j, 0, {"tp": pair_col}).start()

        hosts(run)

    def tok_relay(j):
        def run():
            for g in range(1, groups):
                index = far(g) * PARTS + j
                tok_arrive(index)
                tok_copy(index, j, groups - 1 + g, {"tp": pair_col}).start()

        hosts(run)

    def tok_rest():
        def run():
            for j in range(PARTS):
                tok_arrive(pair_col * PARTS + j)
                for g in range(1, groups):
                    tok_arrive(far_pair(g) * PARTS + j)

        hosts(run)

    def multiply(piece, source, base, size):
        at = slice(base, base + size)
        if wide:
            x = tok_ref[at, pl.ds(pl.multiple_of(source * rows, rows), rows)]
        else:
            x = tok_ref[source, at]
        if piece == 0:
            gate_acc[at] += lax.dot_general(
                x, gate_buf[source], (((1,), (1,)), ((), ())), preferred_element_type=jnp.float32
            )
        elif piece >= 3 * HALVES:
            cols = slice((piece - 3 * HALVES) * quarter, (piece - 3 * HALVES + 1) * quarter)
            acc[3 * HALVES - 1, at, cols] += jnp.dot(
                x, kvq_buf[3 * HALVES - 1, source, :, cols], preferred_element_type=jnp.float32
            )
        else:
            acc[piece - 1, at] += jnp.dot(
                x, kvq_buf[piece - 1, source], preferred_element_type=jnp.float32
            )

    def product(piece, source, part):
        if part == "own":
            multiply(piece, source, 0, count)
        elif part == "guest":
            hosts(lambda: multiply(piece, source, count, count))
        elif all_hosts:
            multiply(piece, source, 0, 2 * count)
        else:

            @pl.when(is_host)
            def _():
                multiply(piece, source, 0, 2 * count)

            @pl.when(jnp.logical_not(is_host))
            def _():
                multiply(piece, source, 0, count)

    def mine(number, part):
        for piece in PHASES[number]:
            product(piece, me, part)

    def middles(number, part):
        def run(origin, onward, target):
            for piece in PHASES[number]:
                product(piece, origin * CROSS + b, part)

        each_middle(run)

    def outside(number, which, part):
        origin = ends()[which][0]
        for piece in PHASES[number]:
            if piece in EARLY:

                @pl.loop(0, CROSS)
                def _(side):
                    product(piece, origin * CROSS + side, part)

            else:
                product(piece, origin * CROSS + b, part)

    def crossed_mine(number, part):
        for piece in PHASES[number]:
            arrive(piece, peer)
            product(piece, peer, part)

    def crossed(number, part):
        pieces = PHASES[number]

        def run(origin, onward, target):
            for piece in pieces:
                source = origin * CROSS + (1 - b)
                arrive(piece, source)
                product(piece, source, part)

        each_middle(run)

    def crossed_outside(number, which, part):
        for piece in PHASES[number]:
            if piece not in EARLY:
                source = ends()[which][0] * CROSS + (1 - b)
                arrive(piece, source)
                product(piece, source, part)

    def guests(number, rest=True):
        pieces = PHASES[number]

        def run():
            if rest:

                @pl.loop(0, seq)
                def _(source):
                    for piece in pieces:
                        multiply(piece, source, count, count)

            else:

                @pl.loop(CROSS, seq - CROSS)
                def _(source):
                    for piece in pieces:
                        multiply(piece, source, count, count)

        hosts(run)

    trips = 2 if all_hosts else 1 + is_host.astype(jnp.int32)
    first_group = jnp.where(is_low, 1, 0)
    second_group = 1 - first_group

    def token_rows(w, start, size):
        return pl.ds(pl.multiple_of(w * count + start, block), size)

    def decays():
        @pl.loop(0, trips)
        def _(w):
            logits = jnp.concatenate(
                [
                    gate_acc[token_rows(w, 0, count)],
                    jnp.zeros((count, 128 - gate_acc.shape[1]), jnp.float32),
                ],
                axis=1,
            ).T[:8]
            soft = jnp.maximum(logits, 0.0) + jnp.log1p(jnp.exp(-jnp.abs(logits)))
            head_row = lax.broadcasted_iota(jnp.int32, soft.shape, 0)
            rate = jnp.zeros(soft.shape, jnp.float32)
            for head in range(heads):
                rate = jnp.where(head_row == head, rate_ref[head], rate)
            total = -rate * soft
            lane = lax.broadcasted_iota(jnp.int32, total.shape, 1)
            reach = 1
            while reach < count:
                total = total + jnp.where(lane >= reach, pltpu.roll(total, reach, 1), 0.0)
                reach *= 2
            wrow[w] = total
            wcol[w] = jnp.concatenate([total, jnp.zeros((120, count), jnp.float32)], axis=0).T

    class local_copy:
        def __init__(self, h, slot, group):
            pairs = ((state_wire, state_peer), (total_mine, total_peer))
            self.copies = [
                pltpu.make_async_remote_copy(
                    src_ref=source.at[group, h],
                    dst_ref=target.at[slot, h],
                    send_sem=local_send.at[n, slot, h],
                    recv_sem=local_recv.at[n, slot, h],
                    device_id={"seq": peer},
                    device_id_type=MESH,
                )
                for n, (source, target) in enumerate(pairs)
            ]

        def start(self):
            for one in self.copies:
                one.start()

        def wait_recv(self):
            for one in self.copies:
                one.wait_recv()

        def wait_send(self):
            for one in self.copies:
                one.wait_send()

    def local_state(h):
        @pl.loop(0, trips)
        def _(w):
            for j in range(per_half):
                head = h * per_half + j
                cols = slice(j * head_size, (j + 1) * head_size)
                within = wcol[w, :, head : head + 1]
                final = wcol[w, count - 1 : count, head : head + 1]
                at = token_rows(w, 0, count)
                key = acc[3 * h, at, cols].astype(jnp.bfloat16).astype(jnp.float32)
                scaled = (jnp.exp(final - within) * key).astype(jnp.bfloat16)
                value = acc[3 * h + 1, at, cols].astype(jnp.bfloat16)
                local = lax.dot_general(
                    scaled, value, (((0,), (0,)), ((), ())), preferred_element_type=jnp.float32
                )
                state_mine[w, h, j * head_size : (j + 1) * head_size] = local
                state_wire[w, h, j * head_size : (j + 1) * head_size] = local.astype(jnp.bfloat16)
                total_mine[w, h, j : j + 1] = jnp.broadcast_to(final, (1, head_size))

        local_copy(h, 0, first_group).start()
        hosts(lambda: local_copy(h, 1, second_group).start())

    def line_state(h):
        return pltpu.make_async_remote_copy(
            src_ref=state_next.at[h],
            dst_ref=state_in.at[h],
            send_sem=state_send.at[h],
            recv_sem=state_recv.at[h],
            device_id={"seq": me + CROSS},
            device_id_type=MESH,
        )

    def chain(h, low):
        pl.when(is_low if low else jnp.logical_not(is_low))(lambda: chain_step(h, low))

    def chain_step(h, low):
        if low:
            state_in[h] = jnp.zeros(state_in.shape[1:], jnp.float32)
        else:
            line_state(h).wait_recv()

        spans = [slice(j * head_size, (j + 1) * head_size) for j in range(per_half)]

        def step(state, j, slot, group, peers):
            own = (total_mine[group, h, j : j + 1], state_mine[group, h, spans[j]])
            other = (
                total_peer[slot, h, j : j + 1],
                state_peer[slot, h, spans[j]].astype(jnp.float32),
            )
            total = jnp.where(peers, other[0], own[0])
            return jnp.exp(total) * state + jnp.where(peers, other[1], own[1])

        def pass_group(slot, group):
            local_copy(h, slot, group).wait_recv()
            for j, at in enumerate(spans):
                state = state_in[h, at] if slot == 0 else state_next[h, at]
                middle_state = step(state, j, slot, group, b == 1)
                state_pre[group, h, at] = jnp.where(b == 1, middle_state, state).astype(
                    jnp.bfloat16
                )
                state_next[h, at] = step(middle_state, j, slot, group, b == 0)

        pass_group(0, first_group)
        hosts(lambda: pass_group(1, second_group))

        @pl.when(up_works)
        def _():
            line_state(h).start()

    def block_rows(i):
        return pl.ds(i * block if isinstance(i, int) else pl.multiple_of(i * block, block), block)

    def normed_copy(u, i, source, send, target):
        h, start, size, _ = units[u]
        ref = normed_buf.at[h, source, block_rows(i), pl.ds(start, size)]
        return pltpu.make_async_remote_copy(
            src_ref=ref,
            dst_ref=ref,
            send_sem=normed_send.at[u, i, send],
            recv_sem=normed_recv.at[u, i, source],
            device_id={"tp": target},
            device_id_type=MESH,
        )

    def guest_copy(u, i):
        h, start, size, _ = units[u]
        return pltpu.make_async_remote_copy(
            src_ref=normed_buf.at[h, tp, block_rows(i), pl.ds(start, size)],
            dst_ref=normed_buf.at[h, col, block_rows(i), pl.ds(start, size)],
            send_sem=guest_send.at[u, i],
            recv_sem=normed_recv.at[u, i, col],
            device_id={"seq": partner},
            device_id_type=MESH,
        )

    def share(u, i):
        for g in range(1, groups):
            normed_copy(u, i, col, g, far(g)).start()
        normed_copy(u, i, col, 0, pair_col).start()

    def relay(u, i):
        for g in range(1, groups):
            normed_copy(u, i, far(g), 0, pair_col).wait_recv()
            normed_copy(u, i, far(g), groups - 1 + g, pair_col).start()

    def attention(u):
        h, _, _, members = units[u]

        @pl.loop(0, trips)
        def _(n):
            w = trips - 1 - n
            slot = jnp.where(w == 0, col, tp)
            for i in range(blocks):
                upto = (i + 1) * block
                row = i * block + lax.broadcasted_iota(jnp.int32, (block, upto), 0)
                causal = lax.broadcasted_iota(jnp.int32, (block, upto), 1) <= row
                t_at = token_rows(w, i * block, block)
                s_at = token_rows(w, 0, upto)
                for j in members:
                    head = h * per_half + j
                    cols = slice(j * head_size, (j + 1) * head_size)
                    query = acc[3 * h + 2, t_at, cols].astype(jnp.bfloat16)
                    key = acc[3 * h, s_at, cols].astype(jnp.bfloat16)
                    value = acc[3 * h + 1, s_at, cols].astype(jnp.bfloat16)
                    within = wcol[w, i * block : (i + 1) * block, head : head + 1]
                    scores = lax.dot_general(
                        query, key, (((1,), (1,)), ((), ())), preferred_element_type=jnp.float32
                    )
                    gap = within - wrow[w, head : head + 1, :upto]
                    attn = jnp.where(causal, scores * jnp.exp(jnp.where(causal, gap, 0.0)), 0.0)
                    local = jnp.dot(
                        attn.astype(jnp.bfloat16), value, preferred_element_type=jnp.float32
                    )
                    scaled = (jnp.exp(within) * query.astype(jnp.float32)).astype(jnp.bfloat16)
                    state = state_pre[w, h, j * head_size : (j + 1) * head_size]
                    head_out = local + jnp.dot(scaled, state, preferred_element_type=jnp.float32)
                    square = jnp.mean(head_out * head_out, axis=-1, keepdims=True)
                    gain = gain_ref[:, head * head_size : (head + 1) * head_size]
                    normed_buf[h, slot, i * block : (i + 1) * block, cols] = (
                        head_out * lax.rsqrt(square + 1e-05) * gain
                    ).astype(jnp.bfloat16)

                @pl.when(w == 0)
                def _():
                    share(u, i)

                @pl.when(w == 1)
                def _():
                    guest_copy(u, i).start()

    def settle(h):
        mine = [u for u in range(len(units)) if units[u][0] == h]

        def mix(i, source):
            depth = pl.ds(pl.multiple_of((source * HALVES + h) * half, half), half)
            return jnp.dot(
                normed_buf[h, source, block_rows(i)],
                out_buf[depth, :],
                preferred_element_type=jnp.float32,
            )

        @pl.loop(0, blocks)
        def _(i):
            at = block_rows(i)
            total = mix(i, col)
            for u in mine:
                normed_copy(u, i, pair_col, 0, pair_col).wait_recv()
            total = total + mix(i, pair_col)
            for g in range(1, groups):
                total = total + mix(i, far(g))
                for u in mine:
                    normed_copy(u, i, far_pair(g), 0, pair_col).wait_recv()
                total = total + mix(i, far_pair(g))
            if h == 0:
                out_acc[at, :] = total
            else:
                mixed_ref[at, :] = (out_acc[at, :] + total).astype(jnp.bfloat16)

    def relays(u):
        @pl.loop(0, blocks)
        def _(i):
            relay(u, i)

    def end_drain():
        for pieces in PHASES:
            for piece in pieces:
                copy(piece, me, send_own.at[piece, 1], peer).wait_send()
                if piece in EARLY:
                    copy(piece, me, send_own.at[piece, 0], peer).wait_send()
                    copy(piece, peer, send_line.at[piece, peer], peer).wait_send()
        for j in range(PARTS):
            tok_copy(col * PARTS + j, j, 0, {"seq": partner}, True).wait_send()

    def worker_drain():
        def host_drain():
            for j in range(PARTS):
                for k in range(tp - 1):
                    tok_copy(col * PARTS + j, j, k, {"tp": pair_col}).wait_send()

        hosts(host_drain)
        for h in range(HALVES):

            local_copy(h, 0, first_group).wait_send()
            hosts(lambda: local_copy(h, 1, second_group).wait_send())

            @pl.when(up_works)
            def _():
                line_state(h).wait_send()

        for pieces in PHASES:
            for piece in pieces:
                copy(piece, me, send_own.at[piece, 0], peer).wait_send()

                @pl.when(up_works)
                def _():
                    copy(piece, me, send_own.at[piece, 1], peer).wait_send()

                @pl.when(down_works)
                def _():
                    copy(piece, me, send_own.at[piece, 2], peer).wait_send()

                for origin, onward, _ in ends():
                    source, other = origin * CROSS + b, origin * CROSS + (1 - b)

                    @pl.when(onward)
                    def _():
                        copy(piece, source, send_line.at[piece, source], peer).wait_send()
                        if piece in EARLY:
                            copy(piece, other, send_line.at[piece, other], peer).wait_send()

                    if piece not in EARLY:
                        copy(piece, source, send_peer.at[piece, source], peer).wait_send()

        def run(origin, onward, target):
            source = origin * CROSS + b
            for pieces in PHASES:
                for piece in pieces:
                    copy(piece, source, send_peer.at[piece, source], peer).wait_send()

                    @pl.when(onward)
                    def _():
                        copy(piece, source, send_line.at[piece, source], peer).wait_send()

        each_middle(run)

    @pl.when(is_end)
    def _():
        for j in range(PARTS):
            tok_copy(col * PARTS + j, j, 0, {"seq": partner}, True).start()
        for pieces in PHASES:
            for piece in pieces:
                load_wait(piece)
                if piece in EARLY:
                    copy(piece, me, send_own.at[piece, 0], peer).start()
        for pieces in PHASES:
            for piece in pieces:
                copy(piece, me, send_own.at[piece, 1], partner).start()
                if piece in EARLY:
                    arrive(piece, peer)
                    copy(piece, peer, send_line.at[piece, peer], partner).start()
        out_load.wait()

        def hand_out(u):
            @pl.loop(0, blocks)
            def _(i):
                guest_copy(u, i).wait_recv()
                share(u, i)

        hand_out(0)
        hand_out(1)
        relays(0)
        end_drain()
        hand_out(2)
        relays(1)
        settle(0)
        relays(2)

    @pl.when(is_worker)
    def _():
        ready(0)
        own_cross(0)
        own_line(0)
        tok_spread(0)
        ready(1)
        own_cross(1)
        own_line(1)
        tok_spread(1)
        middle(0)
        tok_relay(0)
        middle(1)
        tok_spread(2)
        ready(2)
        own_line(2)
        tok_spread(3)
        own_cross(2)
        tok_spread(4)
        ready(4)
        gate_acc[...] = jnp.zeros_like(gate_acc)
        acc[...] = jnp.zeros_like(acc)
        tok_load.wait()
        mine(4, "own")
        ready(3)
        own_cross(3)
        own_line(3)
        crossed_mine(1, "own")
        tok_relay(1)
        own_line(4)
        middle(2)
        tok_relay(2)
        ready(5)
        own_line(5)
        tok_spread(5)
        crossed(0, "own")
        middles(0, "own")
        ready(6)
        own_line(6)
        tok_relay(3)
        middle(3)
        tok_spread(6)
        outer(0, 0, 0)
        mine(5, "own")
        tok_spread(7)
        crossed_mine(2, "own")
        tok_relay(4)
        tok_relay(5)
        mine(1, "own")
        outer(1, 0, 0)
        crossed(1, "own")
        tok_relay(6)
        mine(6, "own")
        tok_relay(7)
        outer(0, 1, 0)
        own_cross(4)
        middles(3, "own")
        middles(2, "own")
        mine(3, "own")
        crossed(3, "own")
        crossed_mine(0, "own")
        tok_rest()
        outer(1, 0, 1)
        outside(1, 0, "both")
        guests(1, False)
        crossed_mine(3, "own")
        outside(0, 1, "own")
        crossed_outside(0, 0, "own")
        outer(2, 0, 0)
        guests(3, False)
        outside(0, 0, "own")
        mine(2, "own")
        outer(1, 1, 1)
        crossed_outside(0, 1, "own")
        outer(1, 1, 0)
        outside(1, 1, "both")
        outer(3, 0, 0)
        guests(0)
        outside(2, 0, "own")
        middles(1, "own")
        mine(0, "own")
        crossed(2, "own")
        outer(2, 1, 0)
        outside(2, 1, "own")
        outer(3, 0, 1)
        decays()
        middle(4)
        crossed_mine(4, "own")
        middles(4, "own")
        local_state(0)
        middle(5)
        crossed_outside(2, 0, "own")
        outer(3, 1, 0)
        middles(5, "own")
        outer(4, 0, 0)
        middle(6)
        outside(3, 0, "both")
        crossed_outside(2, 1, "own")
        guests(2)
        outer(4, 0, 1)
        outside(4, 0, "both")
        outer(3, 1, 1)
        crossed(4, "own")
        outside(3, 1, "both")
        local_state(1)
        outer(4, 1, 0)
        middles(6, "own")
        own_cross(5)
        guests(4, False)
        own_cross(6)
        chain(0, True)
        outer(5, 0, 0)
        outer(5, 0, 1)
        outer(4, 1, 1)
        outside(4, 1, "both")
        chain(0, False)
        attention(0)
        chain(1, True)
        outside(5, 0, "both")
        outer(6, 0, 0)
        crossed_mine(5, "own")
        outer(6, 0, 1)
        outside(6, 0, "both")
        crossed_mine(6, "own")
        outer(5, 1, 1)
        outer(5, 1, 0)
        outside(5, 1, "both")
        crossed(5, "own")
        guests(5, False)
        chain(1, False)
        attention(1)
        crossed(6, "own")
        guests(6, False)
        outer(6, 1, 1)
        outer(6, 1, 0)
        outside(6, 1, "both")
        attention(2)
        relays(0)
        relays(1)
        out_load.wait()
        settle(0)
        worker_drain()
        relays(2)

    settle(1)

    @pl.loop(0, blocks)
    def _(i):
        for u in range(len(units)):
            for k in range(tp - 1):
                normed_copy(u, i, col, k, pair_col).wait_send()

    @pl.when(is_worker)
    def _():
        def run():
            @pl.loop(0, blocks)
            def _(i):
                for u in range(len(units)):
                    guest_copy(u, i).wait_send()

        hosts(run)


def on_device(
    seq,
    tp,
    tokens,
    query_weight,
    key_weight,
    value_weight,
    gate_weight,
    decay_rate,
    norm_gain,
    out_weight,
):
    count = tokens.shape[0]
    rows, width = query_weight.shape
    heads = gate_weight.shape[1]
    half = width // HALVES
    head_size = width // heads
    wide = rows % 128 == 0
    tok = tokens if wide else tokens.reshape(count, seq, rows).transpose(1, 0, 2)
    vmem = pl.BlockSpec(memory_space=pltpu.VMEM)
    smem = pl.BlockSpec(memory_space=pltpu.SMEM)
    hbm = pl.BlockSpec(memory_space=pl.ANY)
    pieces = 3 * HALVES + 2
    blocks = count // 256 if count % 256 == 0 else 1
    dma = pltpu.SemaphoreType.DMA
    deep = head_size * heads // HALVES
    out_width = out_weight.shape[1]
    both = (2 * count, tok.shape[1]) if wide else (seq, 2 * count, rows)
    return pl.pallas_call(
        functools.partial(layer_kernel, seq, tp, heads, wide),
        out_shape=jax.ShapeDtypeStruct((count, out_width), jnp.bfloat16),
        in_specs=[hbm, smem, vmem, hbm, hbm, hbm, hbm, hbm],
        out_specs=vmem,
        scratch_shapes=[
            pltpu.VMEM((seq, 16, rows), jnp.bfloat16),
            pltpu.VMEM((3 * HALVES, seq, rows, half), jnp.bfloat16),
            pltpu.VMEM((2 * count, 16), jnp.float32),
            pltpu.VMEM((3 * HALVES, 2 * count, half), jnp.float32),
            pltpu.VMEM(out_weight.shape, jnp.bfloat16),
            pltpu.VMEM((count, out_width), jnp.float32),
            pltpu.VMEM((2, count, 128), jnp.float32),
            pltpu.VMEM((2, 8, count), jnp.float32),
            pltpu.VMEM((2, HALVES, deep, head_size), jnp.float32),
            pltpu.VMEM((2, HALVES, deep, head_size), jnp.bfloat16),
            pltpu.VMEM((2, HALVES, deep, head_size), jnp.bfloat16),
            pltpu.VMEM((2, HALVES, 8, head_size), jnp.float32),
            pltpu.VMEM((2, HALVES, 8, head_size), jnp.float32),
            pltpu.VMEM((HALVES, deep, head_size), jnp.float32),
            pltpu.VMEM((HALVES, deep, head_size), jnp.float32),
            pltpu.VMEM((2, HALVES, deep, head_size), jnp.bfloat16),
            pltpu.VMEM((HALVES, tp + 1, count, half), jnp.bfloat16),
            pltpu.VMEM(both, jnp.bfloat16),
            dma((pieces + 2,)),
            dma((pieces, 3)),
            dma((pieces, seq)),
            dma((pieces, seq)),
            dma((pieces, seq)),
            dma((PARTS, tp - 1)),
            dma((tp * PARTS,)),
            dma((2, 2, HALVES)),
            dma((2, 2, HALVES)),
            dma((HALVES,)),
            dma((HALVES,)),
            dma((3, blocks, tp - 1)),
            dma((3, blocks, tp)),
            dma((3, blocks)),
            pltpu.VMEM((rows, heads), jnp.bfloat16),
        ],
        compiler_params=pltpu.CompilerParams(
            collective_id=0, has_side_effects=True, vmem_limit_bytes=62 * 1024 * 1024
        ),
    )(tok, decay_rate, norm_gain[None, :], gate_weight, key_weight, value_weight, query_weight, out_weight)


def solution(mesh):
    return jax.shard_map(
        functools.partial(on_device, mesh.shape["seq"], mesh.shape["tp"]),
        mesh=mesh,
        in_specs=(
            P("seq", None),
            P("seq", "tp"),
            P("seq", "tp"),
            P("seq", "tp"),
            P("seq", "tp"),
            P("tp"),
            P("tp"),
            P(None, "tp"),
        ),
        out_specs=P("seq", "tp"),
        check_vma=False,
    )
```
